16 devices in a mesh: dp: 4 (over z, y), tp: 4 (over x, core).
Axes of the slice: x: 2, y: 2, z: 2, core: 2. Of those that a mesh axis runs over, the one named last changes fastest.
Arguments:
- x_tok: bfloat16 [48, 768, 1152], P('dp', 'tp')
- y_cap: bfloat16 [48, 300, 1152], P('dp')
- y_valid: int32 [48, 300], P('dp')
- t_emb: bfloat16 [48, 6912], P('dp')
- mod_table: bfloat16 [6, 1152], replicated
- w_qkv: bfloat16 [1152, 3, 16, 72], P(None, None, 'tp')
- w_proj: bfloat16 [16, 72, 1152], P('tp')
- w_cq: bfloat16 [1152, 16, 72], P(None, 'tp')
- w_ckv: bfloat16 [1152, 2, 16, 72], P(None, None, 'tp')
- w_cproj: bfloat16 [16, 72, 1152], P('tp')
- w_fc1: bfloat16 [1152, 4608], P(None, 'tp')
- w_fc2: bfloat16 [4608, 1152], P('tp')
- d_out: bfloat16 [48, 768, 1152], P('dp', 'tp')
Outputs:
- output 1: bfloat16 [48, 768, 1152], P('dp', 'tp')
- output 2: bfloat16 [48, 768, 1152], P('dp', 'tp')
- output 3: float32 [48, 300, 1152], P('dp')
- output 4: float32 [48, 6912], P('dp')
- output 5: float32 [6, 1152], replicated
- output 6: float32 [1152, 3, 16, 72], P(None, None, 'tp')
- output 7: float32 [16, 72, 1152], P('tp')
- output 8: float32 [1152, 16, 72], P(None, 'tp')
- output 9: float32 [1152, 2, 16, 72], P(None, None, 'tp')
- output 10: float32 [16, 72, 1152], P('tp')
- output 11: float32 [1152, 4608], P(None, 'tp')
- output 12: float32 [4608, 1152], P('tp')
All inputs are finite; a program needn't handle non-finite values.
Results may differ from the reference program's by a relative error of at most 0.0177592.
Values are sent between devices in bfloat16 or wider.
A program may use at most 1 GiB of HBM per device.

```python
import jax
import jax.numpy as jnp
from jax import lax

BATCH = 48
TOKENS = 768
D_MODEL = 1152
HEADS = 16
HEAD_DIM = 72
FF_DIM = 4608
CAP_LEN = 300


def setup_inputs(seed: int = 0) -> dict:
    keys = jax.random.split(jax.random.key(seed), 14)
    fan_model = D_MODEL ** -0.5
    fan_hidden = FF_DIM ** -0.5
    lengths = jax.random.randint(keys[2], (BATCH,), 8, CAP_LEN + 1)
    full_row = jax.random.randint(keys[3], (), 0, BATCH)
    lengths = jnp.where(jnp.arange(BATCH) == full_row, CAP_LEN, lengths)
    y_valid = (jnp.arange(CAP_LEN)[None, :] < lengths[:, None]).astype(jnp.int32)

    def normal(key_index, shape, scale):
        return (scale * jax.random.normal(keys[key_index], shape, jnp.float32)).astype(jnp.bfloat16)

    return {
        'x_tok': normal(0, (BATCH, TOKENS, D_MODEL), 1.0),
        'y_cap': normal(1, (BATCH, CAP_LEN, D_MODEL), 1.0),
        'y_valid': y_valid,
        't_emb': normal(4, (BATCH, 6 * D_MODEL), 0.5),
        'mod_table': normal(5, (6, D_MODEL), 0.5),
        'w_qkv': normal(6, (D_MODEL, 3, HEADS, HEAD_DIM), fan_model),
        'w_proj': normal(7, (HEADS, HEAD_DIM, D_MODEL), fan_model),
        'w_cq': normal(8, (D_MODEL, HEADS, HEAD_DIM), fan_model),
        'w_ckv': normal(9, (D_MODEL, 2, HEADS, HEAD_DIM), fan_model),
        'w_cproj': normal(10, (HEADS, HEAD_DIM, D_MODEL), fan_model),
        'w_fc1': normal(11, (D_MODEL, FF_DIM), fan_model),
        'w_fc2': normal(12, (FF_DIM, D_MODEL), fan_hidden),
        'd_out': normal(13, (BATCH, TOKENS, D_MODEL), 1.0),
    }


def snap_bf16(values):
    return values.astype(jnp.bfloat16).astype(jnp.float32)


def layer_norm(values):
    centered = values - jnp.mean(values, axis=-1, keepdims=True)
    return centered * lax.rsqrt(jnp.mean(centered * centered, axis=-1, keepdims=True) + 1e-6)


def attend(q_heads, k_heads, v_heads, key_bias):
    scores = jnp.einsum('hne,hse->hns', q_heads, k_heads) * (HEAD_DIM ** -0.5) + key_bias
    probs = snap_bf16(jax.nn.softmax(scores, axis=-1))
    return snap_bf16(jnp.einsum('hns,hse->hne', probs, v_heads))


def block_one(x_row, y_row, valid_row, mod_rows, weights):
    w_qkv, w_proj, w_cq, w_ckv, w_cproj, w_fc1, w_fc2 = weights
    shift_msa = mod_rows[0]
    scale_msa = mod_rows[1]
    gate_msa = mod_rows[2]
    shift_mlp = mod_rows[3]
    scale_mlp = mod_rows[4]
    gate_mlp = mod_rows[5]
    mod_in1 = snap_bf16(layer_norm(x_row) * (1.0 + scale_msa) + shift_msa)
    qkv_rows = snap_bf16(jnp.dot(mod_in1, w_qkv.reshape(D_MODEL, 3 * D_MODEL)))
    qkv_heads = qkv_rows.reshape(TOKENS, 3, HEADS, HEAD_DIM).transpose(1, 2, 0, 3)
    att_self = attend(qkv_heads[0], qkv_heads[1], qkv_heads[2], 0.0)
    proj_out = snap_bf16(jnp.dot(att_self.transpose(1, 0, 2).reshape(TOKENS, D_MODEL), w_proj.reshape(D_MODEL, D_MODEL)))
    x_one = x_row + gate_msa * proj_out
    q_cross = snap_bf16(jnp.dot(snap_bf16(x_one), w_cq.reshape(D_MODEL, D_MODEL)))
    q_cross = q_cross.reshape(TOKENS, HEADS, HEAD_DIM).transpose(1, 0, 2)
    kv_cross = snap_bf16(jnp.dot(y_row, w_ckv.reshape(D_MODEL, 2 * D_MODEL)))
    kv_cross = kv_cross.reshape(CAP_LEN, 2, HEADS, HEAD_DIM).transpose(1, 2, 0, 3)
    key_bias = jnp.where(valid_row > 0, 0.0, -1e9)
    att_cross = attend(q_cross, kv_cross[0], kv_cross[1], key_bias)
    cross_out = snap_bf16(jnp.dot(att_cross.transpose(1, 0, 2).reshape(TOKENS, D_MODEL), w_cproj.reshape(D_MODEL, D_MODEL)))
    x_two = x_one + cross_out
    mod_in2 = snap_bf16(layer_norm(x_two) * (1.0 + scale_mlp) + shift_mlp)
    gelu_out = snap_bf16(jax.nn.gelu(jnp.dot(mod_in2, w_fc1), approximate=True))
    mlp_out = snap_bf16(jnp.dot(gelu_out, w_fc2))
    return x_two + gate_mlp * mlp_out


def reference(x_tok, y_cap, y_valid, t_emb, mod_table, w_qkv, w_proj, w_cq, w_ckv, w_cproj, w_fc1, w_fc2, d_out):
    weights = tuple(weight.astype(jnp.float32) for weight in (w_qkv, w_proj, w_cq, w_ckv, w_cproj, w_fc1, w_fc2))
    mod_rows = t_emb.astype(jnp.float32).reshape(BATCH, 6, D_MODEL) + mod_table.astype(jnp.float32)
    block_ckpt = jax.checkpoint(block_one)

    def forward(x_all, y_all, mods_all, weight_set):
        def one_sample(row):
            return block_ckpt(row[0], row[1], row[2], row[3], weight_set)
        return lax.map(one_sample, (x_all, y_all, y_valid, mods_all))

    x_three, pull = jax.vjp(forward, x_tok.astype(jnp.float32), y_cap.astype(jnp.float32), mod_rows, weights)
    d_x, d_y, d_mods, d_weights = pull(d_out.astype(jnp.float32))
    return (x_three.astype(jnp.bfloat16), d_x.astype(jnp.bfloat16), d_y,
            d_mods.reshape(BATCH, 6 * D_MODEL), jnp.sum(d_mods, axis=0),
            d_weights[0], d_weights[1], d_weights[2], d_weights[3], d_weights[4], d_weights[5], d_weights[6])
```

```python
import functools
import jax
import jax.numpy as jnp
from jax import lax
from jax.experimental import pallas as pl
from jax.experimental.pallas import tpu as pltpu
from jax.sharding import PartitionSpec as P

LN_EPS = 1e-6
HEADS = 16
HEAD_DIM = 72
WIN = 256
CHUNK = 256
SCALE = HEAD_DIM ** -0.5
LOG2E = 1.4426950408889634
BF16 = jnp.bfloat16
F32 = jnp.float32


def layer_norm(values):
    centered = values - jnp.mean(values, axis=-1, keepdims=True)
    inv_std = lax.rsqrt(jnp.mean(centered * centered, axis=-1, keepdims=True) + LN_EPS)
    return centered * inv_std, inv_std


def norm_back(normed, inv_std, grad_in):
    return inv_std * (grad_in - jnp.mean(grad_in, axis=-1, keepdims=True)
                      - normed * jnp.mean(grad_in * normed, axis=-1, keepdims=True))


def contract(left, right, left_dim, right_dim):
    return lax.dot_general(left, right, (((left_dim,), (right_dim,)), ((), ())), preferred_element_type=F32)


def head_window(width):
    head = pl.program_id(1)
    tile = jnp.minimum((head * HEAD_DIM) // 128, width // 128 - WIN // 128)
    first = head * HEAD_DIM - tile * 128
    lane = lax.broadcasted_iota(jnp.int32, (1, WIN), 1)
    return pl.multiple_of(tile * 128, 128), (lane >= first) & (lane < first + HEAD_DIM)


def load(ref, at):
    value = ref[:, 0, :, at]
    return value.reshape(-1, value.shape[-1])


def keep_lanes(mask, value):
    return jnp.where(mask, value.astype(F32), 0.0).astype(BF16)


def put(ref, start, mask, value):
    at = pl.ds(pl.multiple_of(start, 128), WIN)
    old = ref[:, 0, :, at]
    ref[:, 0, :, at] = jnp.where(mask, value.reshape(old.shape), old.astype(F32)).astype(BF16)


def fwd_kernel(has_bias, q_ref, k_ref, v_ref, *refs):
    bias_ref = refs[0] if has_bias else None
    o_ref, lse_ref = refs[-2:]
    head = pl.program_id(1)
    start, mask = head_window(o_ref.shape[-1])
    win = pl.ds(start, WIN)
    keys = load(k_ref, win)
    vals = load(v_ref, win)
    query_all = keep_lanes(mask, load(q_ref, win))
    outs = []
    for first in range(0, query_all.shape[0], CHUNK):
        scores = contract(keys, query_all[first:first + CHUNK], 1, 1)
        if has_bias:
            scores = scores + bias_ref[0]
        top = jnp.max(scores, axis=0, keepdims=True)
        probs = jnp.exp2((scores - top) * (SCALE * LOG2E))
        total = jnp.sum(probs, axis=0, keepdims=True)
        probs = (probs * (1.0 / total)).astype(BF16)
        outs.append(contract(probs, vals, 0, 0))
        lse_ref[0, pl.ds(head, 1), pl.ds(first, CHUNK)] = top * (SCALE * LOG2E) + jnp.log2(total)
    put(o_ref, start, mask, jnp.concatenate(outs, axis=0))


def bwd_kernel(has_bias, fused_out, q_ref, k_ref, v_ref, do_ref, lse_ref, *refs):
    bias_ref = refs[0] if has_bias else None
    p_s, ds_s = refs[-2:]
    outs = refs[1:-2] if has_bias else refs[:-2]
    width = q_ref.shape[-1]
    if fused_out:
        dq_ref = dk_ref = dv_ref = outs[0]
        dq_off, dk_off, dv_off = 0, width, 2 * width
    else:
        dq_ref, dk_ref, dv_ref = outs[0], outs[1], outs[1]
        dq_off, dk_off, dv_off = 0, 0, width
    head = pl.program_id(1)
    start, mask = head_window(width)
    win = pl.ds(start, WIN)
    keys = load(k_ref, win)
    vals = load(v_ref, win)
    query_all = keep_lanes(mask, load(q_ref, win))
    dout_all = keep_lanes(mask, load(do_ref, win))
    for first in range(0, query_all.shape[0], CHUNK):
        rows = pl.ds(first, CHUNK)
        scores = contract(keys, query_all[first:first + CHUNK], 1, 1)
        if has_bias:
            scores = scores + bias_ref[0]
        probs = jnp.exp2(scores * (SCALE * LOG2E) - lse_ref[0, pl.ds(head, 1), rows])
        d_probs = contract(vals, dout_all[first:first + CHUNK], 1, 1)
        delta = jnp.sum(probs * d_probs, axis=0, keepdims=True)
        p_s[:, rows] = probs.astype(BF16)
        ds_s[:, rows] = (probs * (d_probs - delta)).astype(BF16)
    put(dv_ref, start + dv_off, mask, contract(p_s[...], dout_all, 1, 0))
    put(dk_ref, start + dk_off, mask, contract(ds_s[...], query_all, 1, 0) * SCALE)
    put(dq_ref, start + dq_off, mask, contract(ds_s[...], keys, 0, 0) * SCALE)


def sample_spec(array, width, column):
    return pl.BlockSpec((array.shape[0], 1, array.shape[2], width), lambda b, h: (0, b, 0, column))


def attn_fwd(q_arr, q_col, kv_arr, k_col, v_col, bias):
    pieces, batch, rows = q_arr.shape[:3]
    width = HEADS * HEAD_DIM
    tokens = pieces * rows
    n_keys = kv_arr.shape[0] * kv_arr.shape[2]
    args = [q_arr, kv_arr, kv_arr] + ([bias] if bias is not None else [])
    in_specs = [sample_spec(q_arr, width, q_col), sample_spec(kv_arr, width, k_col), sample_spec(kv_arr, width, v_col)]
    if bias is not None:
        in_specs.append(pl.BlockSpec((1, n_keys, 1), lambda b, h: (b, 0, 0)))
    flops = 2 * 2 * batch * HEADS * tokens * n_keys * 128
    return pl.pallas_call(
        functools.partial(fwd_kernel, bias is not None),
        grid=(batch, HEADS),
        in_specs=in_specs,
        out_specs=[sample_spec(q_arr, width, 0), pl.BlockSpec((1, HEADS, tokens), lambda b, h: (b, 0, 0))],
        out_shape=[jax.ShapeDtypeStruct((pieces, batch, rows, width), BF16),
                   jax.ShapeDtypeStruct((batch, HEADS, tokens), F32)],
        compiler_params=pltpu.CompilerParams(dimension_semantics=('arbitrary', 'arbitrary'),
                                             vmem_limit_bytes=48 * 2 ** 20),
        cost_estimate=pl.CostEstimate(flops=flops, transcendentals=batch * HEADS * tokens * n_keys,
                                      bytes_accessed=2 * batch * width * 2 * (tokens + n_keys)),
        name='attn_fwd',
    )(*args)


def attn_bwd(q_arr, q_col, kv_arr, k_col, v_col, d_att, lse, bias, fused_out):
    pieces, batch, rows = q_arr.shape[:3]
    width = HEADS * HEAD_DIM
    tokens = pieces * rows
    n_keys = kv_arr.shape[0] * kv_arr.shape[2]
    args = [q_arr, kv_arr, kv_arr, d_att, lse] + ([bias] if bias is not None else [])
    in_specs = [sample_spec(q_arr, width, q_col), sample_spec(kv_arr, width, k_col), sample_spec(kv_arr, width, v_col),
                sample_spec(d_att, width, 0), pl.BlockSpec((1, HEADS, tokens), lambda b, h: (b, 0, 0))]
    if bias is not None:
        in_specs.append(pl.BlockSpec((1, n_keys, 1), lambda b, h: (b, 0, 0)))
    outs = [(q_arr, 3 * width)] if fused_out else [(q_arr, width), (kv_arr, 2 * width)]
    flops = 2 * 5 * batch * HEADS * tokens * n_keys * 128
    return pl.pallas_call(
        functools.partial(bwd_kernel, bias is not None, fused_out),
        grid=(batch, HEADS),
        in_specs=in_specs,
        out_specs=[sample_spec(array, lanes, 0) for array, lanes in outs],
        out_shape=[jax.ShapeDtypeStruct(array.shape[:3] + (lanes,), BF16) for array, lanes in outs],
        scratch_shapes=[pltpu.VMEM((n_keys, tokens), BF16), pltpu.VMEM((n_keys, tokens), BF16)],
        compiler_params=pltpu.CompilerParams(dimension_semantics=('arbitrary', 'arbitrary'),
                                             vmem_limit_bytes=58 * 2 ** 20),
        cost_estimate=pl.CostEstimate(flops=flops, transcendentals=batch * HEADS * tokens * n_keys,
                                      bytes_accessed=2 * batch * width * 4 * (tokens + n_keys)),
        name='attn_bwd',
    )(*args)


def grad_kernel(left_ref, right_ref, out_ref):
    part = contract(left_ref[...], right_ref[...], 0, 0).reshape(out_ref.shape)

    @pl.when(pl.program_id(1) == 0)
    def _():
        out_ref[...] = part

    @pl.when(pl.program_id(1) != 0)
    def _():
        out_ref[...] += part


def head_grad(left, right):
    width = HEADS * HEAD_DIM
    left = left.reshape(-1, left.shape[-1])
    right = right.reshape(-1, right.shape[-1])
    steps = 3
    block = left.shape[0] // steps
    parts = left.shape[1] // width
    shape = (2, 2, parts, width // 4, right.shape[1])
    return pl.pallas_call(
        grad_kernel,
        grid=(parts, steps),
        in_specs=[pl.BlockSpec((block, width), lambda k, t: (t, k)),
                  pl.BlockSpec((block, right.shape[1]), lambda k, t: (t, 0))],
        out_specs=pl.BlockSpec((2, 2, 1) + shape[3:], lambda k, t: (0, 0, k, 0, 0)),
        out_shape=jax.ShapeDtypeStruct(shape, F32),
        compiler_params=pltpu.CompilerParams(dimension_semantics=('arbitrary', 'arbitrary'),
                                             vmem_limit_bytes=48 * 2 ** 20),
        cost_estimate=pl.CostEstimate(flops=2 * left.shape[0] * left.shape[1] * right.shape[1], transcendentals=0,
                                      bytes_accessed=2 * left.size + 2 * right.size + 4 * left.shape[1] * right.shape[1]),
        name='head_grad',
    )(left, right).reshape(2, 2, -1, right.shape[1])


def solution(mesh):
    in_specs = (P('dp', 'tp', None), P('dp', None, None), P('dp', None), P('dp', None), P(None, None),
                P(None, None, 'tp', None), P('tp', None, None), P(None, 'tp', None), P(None, None, 'tp', None),
                P('tp', None, None), P(None, 'tp'), P('tp', None), P('dp', 'tp', None))
    out_specs = (P('dp', 'tp', None), P('dp', 'tp', None), P('dp', None, None), P('dp', None), P(None, None),
                 P(None, None, 'tp', None), P('tp', None, None), P(None, 'tp', None), P(None, None, 'tp', None),
                 P('tp', None, None), P(None, 'tp'), P('tp', None))

    def swap_core(values):
        return lax.ppermute(values, 'tp', [(0, 1), (1, 0), (2, 3), (3, 2)])

    def swap_chip(values):
        return lax.ppermute(values, 'tp', [(0, 2), (2, 0), (1, 3), (3, 1)])

    def with_core(shard, chip, axis):
        return jnp.concatenate([shard, chip, swap_core(shard), swap_core(chip)], axis=axis)

    tie = lax.optimization_barrier

    def local_step(x_tok, y_cap, y_valid, t_emb, mod_table, w_qkv, w_proj, w_cq, w_ckv, w_cproj, w_fc1, w_fc2, d_out):
        width = x_tok.shape[-1]
        me = lax.axis_index('tp')
        batch = x_tok.shape[0] // 4
        rows = x_tok.shape[1]
        local = w_proj.shape[0] * w_proj.shape[1]

        def exchange(values):
            return lax.all_to_all(values, 'tp', split_axis=0, concat_axis=0, tiled=True)

        def own(values):
            return lax.dynamic_slice_in_dim(values, me * batch, batch, axis=0)

        x_own = exchange(x_tok.reshape(4, batch, rows, width))
        qkv_s = w_qkv.transpose(1, 2, 3, 0).reshape(3, local, width)
        qkv_c = swap_chip(qkv_s)
        qkv_w = with_core(qkv_s, qkv_c, 1).reshape(3 * width, width)
        x_own, qkv_w, mid_s = tie((x_own, qkv_w, (
            w_proj.reshape(local, width), w_cq.transpose(1, 2, 0).reshape(local, width),
            w_ckv.transpose(1, 2, 3, 0).reshape(2, local, width), w_cproj.reshape(local, width))))
        mid_c = tuple(swap_chip(shard) for shard in mid_s)
        mid_c, fc1_s, fc2_s = tie((mid_c, w_fc1, w_fc2))
        proj_w, cq_w, ckv_w, cproj_w = (with_core(s, c, s.ndim - 2) for s, c in zip(mid_s, mid_c))
        ckv_w = ckv_w.reshape(2 * width, width)
        fc1_c, fc2_c = swap_chip(fc1_s), swap_chip(fc2_s)
        fc1_c, fc2_c, d_tok = tie((fc1_c, fc2_c, d_out))
        d_own = exchange(d_tok.reshape(4, batch, rows, width))
        fc1_w = with_core(fc1_s, fc1_c, 1)
        fc2_w = with_core(fc2_s, fc2_c, 0)

        y_own = own(y_cap)
        n_cap = y_own.shape[1]
        n_pad = -n_cap % 16
        y_own = jnp.pad(y_own, ((0, 0), (0, n_pad), (0, 0)))[None]
        valid = jnp.pad(own(y_valid), ((0, 0), (0, n_pad)))
        key_bias = jnp.where(valid > 0, 0.0, -1e30)[:, :, None].astype(F32)
        mod_rows = own(t_emb).astype(F32).reshape(batch, 6, width) + mod_table.astype(F32)
        shift_msa, scale_msa, gate_msa, shift_mlp, scale_mlp, gate_mlp = (mod_rows[:, i, None, :] for i in range(6))

        def dense(values, weight, dim):
            return contract(values.reshape(-1, values.shape[-1]), weight, 1, dim).reshape(
                values.shape[:-1] + (weight.shape[1 - dim],))

        def outer(left, right):
            return contract(left.reshape(-1, left.shape[-1]), right.reshape(-1, right.shape[-1]), 0, 0)

        def over_tokens(values):
            return jnp.sum(values, axis=(0, 2))

        x_res = x_own.astype(F32)
        norm1, inv1 = layer_norm(x_res)
        mod_in1 = (norm1 * (1.0 + scale_msa) + shift_msa).astype(BF16)
        qkv = dense(mod_in1, qkv_w, 1).astype(BF16)
        att_self, lse_self = attn_fwd(qkv, 0, qkv, 1, 2, None)
        proj_out = dense(att_self, proj_w, 0).astype(BF16).astype(F32)
        x_one = x_res + gate_msa * proj_out
        cross_in = x_one.astype(BF16)
        q_cross = dense(cross_in, cq_w, 1).astype(BF16)
        kv_cross = dense(y_own, ckv_w, 1).astype(BF16)
        att_cross, lse_cross = attn_fwd(q_cross, 0, kv_cross, 0, 1, key_bias)
        cross_out = dense(att_cross, cproj_w, 0).astype(BF16).astype(F32)
        x_two = x_one + cross_out
        norm2, inv2 = layer_norm(x_two)
        mod_in2 = (norm2 * (1.0 + scale_mlp) + shift_mlp).astype(BF16)
        hidden = dense(mod_in2, fc1_w, 0)
        gelu_out, gelu_pull = jax.vjp(functools.partial(jax.nn.gelu, approximate=True), hidden)
        gelu_out = gelu_out.astype(BF16)

        d_three = d_own.astype(F32)
        d_mlp = (gate_mlp * d_three).astype(BF16)
        d_gelu = dense(d_mlp, fc2_w, 1).astype(BF16)
        d_hidden = gelu_pull(d_gelu.astype(F32))[0].astype(BF16)
        half = gelu_out.shape[-1] // 2
        gelu_out, d_hidden, d_mlp = tie((gelu_out, d_hidden, d_mlp))
        g2 = outer(gelu_out, d_mlp)
        send2 = g2[half:]
        d_hidden, g2, send2 = tie((d_hidden, g2, send2))
        got2 = swap_core(send2)
        g1 = outer(mod_in2, d_hidden)
        send1 = g1[:, half:]
        d_hidden, g1, send1, got2 = tie((d_hidden, g1, send1, got2))
        got1 = swap_core(send1)
        part2 = lax.psum_scatter((g2[:half] + got2).reshape(2, width, width), 'dp', scatter_dimension=1, tiled=True)
        d_mod2 = dense(d_hidden, fc1_w, 1).astype(BF16).astype(F32)
        d_mod2, got1 = tie((d_mod2, got1))
        chip1 = swap_chip(g1[:, width:half] + got1[:, width:])
        d_scale_mlp = over_tokens(d_mod2 * norm2)
        d_shift_mlp = over_tokens(d_mod2)
        d_two = d_three + norm_back(norm2, inv2, d_mod2 * (1.0 + scale_mlp))

        d_cross = d_two.astype(BF16)
        d_att_c = dense(d_cross, cproj_w, 1).astype(BF16)
        dq_cross, d_kv_cross = attn_bwd(q_cross, 0, kv_cross, 0, 1, d_att_c, lse_cross, key_bias, False)
        dq_cross, d_kv_cross, part2 = tie((dq_cross, d_kv_cross, part2))
        sum2 = part2[0] + swap_chip(part2[1])
        d_xc = dense(dq_cross, cq_w, 0).astype(BF16).astype(F32)
        d_one = d_two + d_xc
        dy_own = dense(d_kv_cross, ckv_w, 0)[0, :, :n_cap]
        d_proj = (gate_msa * d_one).astype(BF16)
        mid = [head_grad(att_self, d_proj), head_grad(att_cross, d_cross), head_grad(dq_cross, cross_in),
               head_grad(d_kv_cross, y_own)]
        mid_send = jnp.concatenate([grad[1] for grad in mid], axis=1)
        d_proj, mid, mid_send, dy_own, sum2, chip1 = tie((d_proj, mid, mid_send, dy_own, sum2, chip1))
        mid_got = swap_core(mid_send)
        g_fc2 = lax.all_gather(sum2, 'dp', axis=0, tiled=True)
        g_fc1 = lax.psum(g1[:, :width] + got1[:, :width] + chip1, 'dp')
        dy_c = swap_chip(dy_own)
        d_gate_msa = over_tokens(d_one * proj_out)
        d_att_s = dense(d_proj, proj_w, 1).astype(BF16)
        d_att_s, mid_got = tie((d_att_s, mid_got))
        mid_part = lax.psum_scatter(jnp.concatenate([grad[0] for grad in mid], axis=1) + mid_got, 'dp',
                                    scatter_dimension=1, tiled=True)
        (d_qkv,) = attn_bwd(qkv, 0, qkv, 1, 2, d_att_s, lse_self, None, True)
        grad_qkv = head_grad(d_qkv, mod_in1)
        d_qkv, grad_qkv, dy_c, g_fc2, g_fc1, gelu_late = tie((d_qkv, grad_qkv, dy_c, g_fc2, g_fc1, gelu_out))
        qkv_got = swap_core(grad_qkv[1])
        mlp_out = dense(gelu_late, fc2_w, 0).astype(BF16).astype(F32)
        out_own = (x_two + gate_mlp * mlp_out).astype(BF16)
        d_gate_mlp = over_tokens(d_three * mlp_out)
        d_qkv, out_own, qkv_got = tie((d_qkv, out_own, qkv_got))
        qkv_part = lax.psum_scatter(grad_qkv[0] + qkv_got, 'dp', scatter_dimension=1, tiled=True)
        out_tok = exchange(out_own).reshape(x_tok.shape)
        d_mod1 = dense(d_qkv, qkv_w, 0).astype(BF16).astype(F32)
        d_scale_msa = over_tokens(d_mod1 * norm1)
        d_shift_msa = over_tokens(d_mod1)
        dx_own = (d_one + norm_back(norm1, inv1, d_mod1 * (1.0 + scale_msa))).astype(BF16)
        dx_own, mid_part, out_tok, dy_c = tie((dx_own, mid_part, out_tok, dy_c))
        dx_tok = exchange(dx_own).reshape(x_tok.shape)
        dys = [dy_own, swap_core(dy_own), dy_c, swap_core(dy_c)]
        dy_cap = jnp.zeros((4 * batch,) + dy_own.shape[1:], F32)
        for index, piece in enumerate(dys):
            dy_cap = lax.dynamic_update_slice_in_dim(dy_cap, piece, (me ^ index) * batch, axis=0)
        g_mid = lax.all_gather(mid_part[0] + swap_chip(mid_part[1]), 'dp', axis=0, tiled=True)
        g_qkv = lax.all_gather(qkv_part[0] + swap_chip(qkv_part[1]), 'dp', axis=0, tiled=True)

        d_mods = jnp.stack([d_shift_msa, d_scale_msa, d_gate_msa, d_shift_mlp, d_scale_mlp, d_gate_mlp], axis=1)
        all_mods = lax.all_gather(d_mods, ('dp', 'tp'), axis=0, tiled=True)
        d_table = jnp.sum(all_mods, axis=0)
        dt_emb = lax.dynamic_slice_in_dim(all_mods, lax.axis_index('dp') * 4 * batch, 4 * batch, axis=0)
        dt_emb = dt_emb.reshape(4 * batch, 6 * width)
        n_heads = local // HEAD_DIM

        def heads(grad, lead):
            return grad.reshape(lead, n_heads, HEAD_DIM, width)

        g_proj, g_cproj, g_cq, g_ckv = (g_mid[i * local:(i + count) * local]
                                        for i, count in ((0, 1), (1, 1), (2, 1), (3, 2)))
        return (out_tok, dx_tok, dy_cap, dt_emb, d_table,
                heads(g_qkv, 3).transpose(3, 0, 1, 2), heads(g_proj, 1)[0], heads(g_cq, 1)[0].transpose(2, 0, 1),
                heads(g_ckv, 2).transpose(3, 0, 1, 2), heads(g_cproj, 1)[0], g_fc1, g_fc2)

    return jax.shard_map(local_step, mesh=mesh, in_specs=in_specs, out_specs=out_specs, check_vma=False)
```

```python
import functools
import jax
import jax.numpy as jnp
from jax import lax
from jax.experimental import pallas as pl
from jax.experimental.pallas import tpu as pltpu
from jax.sharding import PartitionSpec as P

LN_EPS = 1e-6
HEADS = 16
HEAD_DIM = 72
WIN = 256
CHUNK = 256
HEADS_PER_STEP = 2
SCALE = HEAD_DIM ** -0.5
LOG2E = 1.4426950408889634
BF16 = jnp.bfloat16
F32 = jnp.float32


def layer_norm(values):
    centered = values - jnp.mean(values, axis=-1, keepdims=True)
    inv_std = lax.rsqrt(jnp.mean(centered * centered, axis=-1, keepdims=True) + LN_EPS)
    return centered * inv_std, inv_std


def norm_back(normed, inv_std, grad_in):
    return inv_std * (grad_in - jnp.mean(grad_in, axis=-1, keepdims=True)
                      - normed * jnp.mean(grad_in * normed, axis=-1, keepdims=True))


def contract(left, right, left_dim, right_dim):
    return lax.dot_general(left, right, (((left_dim,), (right_dim,)), ((), ())), preferred_element_type=F32)


def head_window(head, width):
    tile = jnp.minimum((head * HEAD_DIM) // 128, width // 128 - WIN // 128)
    first = head * HEAD_DIM - tile * 128
    lane = lax.broadcasted_iota(jnp.int32, (1, WIN), 1)
    return pl.multiple_of(tile * 128, 128), (lane >= first) & (lane < first + HEAD_DIM)


def load(ref, at):
    value = ref[:, 0, :, at]
    return value.reshape(-1, value.shape[-1])


def keep_lanes(mask, value):
    return value * mask.astype(F32).astype(BF16)


def put(ref, start, mask, value):
    at = pl.ds(pl.multiple_of(start, 128), WIN)
    old = ref[:, 0, :, at]
    ref[:, 0, :, at] = jnp.where(mask, value.reshape(old.shape), old.astype(F32)).astype(BF16)


def fwd_kernel(has_bias, q_ref, k_ref, v_ref, *refs):
    bias_ref = refs[0] if has_bias else None
    o_ref, lse_ref = refs[-2:]
    for sub in range(HEADS_PER_STEP):
        head = pl.program_id(1) * HEADS_PER_STEP + sub
        start, mask = head_window(head, o_ref.shape[-1])
        win = pl.ds(start, WIN)
        keys = load(k_ref, win)
        vals = load(v_ref, win)
        query_all = keep_lanes(mask, load(q_ref, win))
        outs = []
        for first in range(0, query_all.shape[0], CHUNK):
            scores = contract(query_all[first:first + CHUNK], keys, 1, 1)
            if has_bias:
                scores = scores + bias_ref[0]
            top = jnp.max(scores, axis=1, keepdims=True)
            probs = jnp.exp2((scores - top) * (SCALE * LOG2E))
            total = jnp.sum(probs, axis=1, keepdims=True)
            outs.append(contract(probs.astype(BF16), vals, 1, 0) * (1.0 / total))
            lse = top * (SCALE * LOG2E) + jnp.log2(total)
            lse_ref[0, pl.ds(head, 1), pl.ds(first, CHUNK)] = jnp.broadcast_to(lse, (CHUNK, 128)).T[:1]
        put(o_ref, start, mask, jnp.concatenate(outs, axis=0))


def bwd_kernel(has_bias, fused_out, q_ref, k_ref, v_ref, do_ref, lse_ref, *refs):
    bias_ref = refs[0] if has_bias else None
    p_s, ds_s = refs[-2:]
    outs = refs[1:-2] if has_bias else refs[:-2]
    width = q_ref.shape[-1]
    if fused_out:
        dq_ref = dk_ref = dv_ref = outs[0]
        dq_off, dk_off, dv_off = 0, width, 2 * width
    else:
        dq_ref, dk_ref, dv_ref = outs[0], outs[1], outs[1]
        dq_off, dk_off, dv_off = 0, 0, width
    for sub in range(HEADS_PER_STEP):
        head = pl.program_id(1) * HEADS_PER_STEP + sub
        start, mask = head_window(head, width)
        win = pl.ds(start, WIN)
        keys = load(k_ref, win)
        vals = load(v_ref, win)
        query_all = keep_lanes(mask, load(q_ref, win))
        dout_all = keep_lanes(mask, load(do_ref, win))
        for first in range(0, query_all.shape[0], CHUNK):
            rows = pl.ds(first, CHUNK)
            scores = contract(keys, query_all[first:first + CHUNK], 1, 1)
            if has_bias:
                scores = scores + bias_ref[0]
            probs = jnp.exp2(scores * (SCALE * LOG2E) - lse_ref[0, pl.ds(head, 1), rows])
            d_probs = contract(vals, dout_all[first:first + CHUNK], 1, 1)
            delta = jnp.sum(probs * d_probs, axis=0, keepdims=True)
            p_s[sub, :, rows] = probs.astype(BF16)
            ds_s[sub, :, rows] = (probs * (d_probs - delta)).astype(BF16)
        put(dv_ref, start + dv_off, mask, contract(p_s[sub], dout_all, 1, 0))
        put(dk_ref, start + dk_off, mask, contract(ds_s[sub], query_all, 1, 0) * SCALE)
        put(dq_ref, start + dq_off, mask, contract(ds_s[sub], keys, 0, 0) * SCALE)


def sample_spec(array, width, column):
    return pl.BlockSpec((array.shape[0], 1, array.shape[2], width), lambda b, h: (0, b, 0, column))


def attn_fwd(q_arr, q_col, kv_arr, k_col, v_col, bias):
    pieces, batch, rows = q_arr.shape[:3]
    width = HEADS * HEAD_DIM
    tokens = pieces * rows
    n_keys = kv_arr.shape[0] * kv_arr.shape[2]
    args = [q_arr, kv_arr, kv_arr] + ([bias] if bias is not None else [])
    in_specs = [sample_spec(q_arr, width, q_col), sample_spec(kv_arr, width, k_col), sample_spec(kv_arr, width, v_col)]
    if bias is not None:
        in_specs.append(pl.BlockSpec((1, 1, n_keys), lambda b, h: (b, 0, 0)))
    flops = 2 * 2 * batch * HEADS * tokens * n_keys * 128
    return pl.pallas_call(
        functools.partial(fwd_kernel, bias is not None),
        grid=(batch, HEADS // HEADS_PER_STEP),
        in_specs=in_specs,
        out_specs=[sample_spec(q_arr, width, 0), pl.BlockSpec((1, HEADS, tokens), lambda b, h: (b, 0, 0))],
        out_shape=[jax.ShapeDtypeStruct((pieces, batch, rows, width), BF16),
                   jax.ShapeDtypeStruct((batch, HEADS, tokens), F32)],
        compiler_params=pltpu.CompilerParams(dimension_semantics=('arbitrary', 'arbitrary'),
                                             vmem_limit_bytes=48 * 2 ** 20),
        cost_estimate=pl.CostEstimate(flops=flops, transcendentals=batch * HEADS * tokens * n_keys,
                                      bytes_accessed=2 * batch * width * 2 * (tokens + n_keys)),
        name='attn_fwd',
    )(*args)


def attn_bwd(q_arr, q_col, kv_arr, k_col, v_col, d_att, lse, bias, fused_out):
    pieces, batch, rows = q_arr.shape[:3]
    width = HEADS * HEAD_DIM
    tokens = pieces * rows
    n_keys = kv_arr.shape[0] * kv_arr.shape[2]
    args = [q_arr, kv_arr, kv_arr, d_att, lse] + ([bias] if bias is not None else [])
    in_specs = [sample_spec(q_arr, width, q_col), sample_spec(kv_arr, width, k_col), sample_spec(kv_arr, width, v_col),
                sample_spec(d_att, width, 0), pl.BlockSpec((1, HEADS, tokens), lambda b, h: (b, 0, 0))]
    if bias is not None:
        in_specs.append(pl.BlockSpec((1, n_keys, 1), lambda b, h: (b, 0, 0)))
    outs = [(q_arr, 3 * width)] if fused_out else [(q_arr, width), (kv_arr, 2 * width)]
    flops = 2 * 5 * batch * HEADS * tokens * n_keys * 128
    return pl.pallas_call(
        functools.partial(bwd_kernel, bias is not None, fused_out),
        grid=(batch, HEADS // HEADS_PER_STEP),
        in_specs=in_specs,
        out_specs=[sample_spec(array, lanes, 0) for array, lanes in outs],
        out_shape=[jax.ShapeDtypeStruct(array.shape[:3] + (lanes,), BF16) for array, lanes in outs],
        scratch_shapes=[pltpu.VMEM((HEADS_PER_STEP, n_keys, tokens), BF16)] * 2,
        compiler_params=pltpu.CompilerParams(dimension_semantics=('arbitrary', 'arbitrary'),
                                             vmem_limit_bytes=58 * 2 ** 20),
        cost_estimate=pl.CostEstimate(flops=flops, transcendentals=batch * HEADS * tokens * n_keys,
                                      bytes_accessed=2 * batch * width * 4 * (tokens + n_keys)),
        name='attn_bwd',
    )(*args)


def grad_kernel(left_ref, right_ref, out_ref):
    part = contract(left_ref[...], right_ref[...], 0, 0).reshape(out_ref.shape)

    @pl.when(pl.program_id(1) == 0)
    def _():
        out_ref[...] = part

    @pl.when(pl.program_id(1) != 0)
    def _():
        out_ref[...] += part


def head_grad(left, right):
    width = HEADS * HEAD_DIM
    left = left.reshape(-1, left.shape[-1])
    right = right.reshape(-1, right.shape[-1])
    steps = 3
    block = left.shape[0] // steps
    parts = left.shape[1] // width
    shape = (2, 2, parts, width // 4, right.shape[1])
    return pl.pallas_call(
        grad_kernel,
        grid=(parts, steps),
        in_specs=[pl.BlockSpec((block, width), lambda k, t: (t, k)),
                  pl.BlockSpec((block, right.shape[1]), lambda k, t: (t, 0))],
        out_specs=pl.BlockSpec((2, 2, 1) + shape[3:], lambda k, t: (0, 0, k, 0, 0)),
        out_shape=jax.ShapeDtypeStruct(shape, F32),
        compiler_params=pltpu.CompilerParams(dimension_semantics=('arbitrary', 'arbitrary'),
                                             vmem_limit_bytes=48 * 2 ** 20),
        cost_estimate=pl.CostEstimate(flops=2 * left.shape[0] * left.shape[1] * right.shape[1], transcendentals=0,
                                      bytes_accessed=2 * left.size + 2 * right.size + 4 * left.shape[1] * right.shape[1]),
        name='head_grad',
    )(left, right).reshape(2, 2, -1, right.shape[1])


def solution(mesh):
    in_specs = (P('dp', 'tp', None), P('dp', None, None), P('dp', None), P('dp', None), P(None, None),
                P(None, None, 'tp', None), P('tp', None, None), P(None, 'tp', None), P(None, None, 'tp', None),
                P('tp', None, None), P(None, 'tp'), P('tp', None), P('dp', 'tp', None))
    out_specs = (P('dp', 'tp', None), P('dp', 'tp', None), P('dp', None, None), P('dp', None), P(None, None),
                 P(None, None, 'tp', None), P('tp', None, None), P(None, 'tp', None), P(None, None, 'tp', None),
                 P('tp', None, None), P(None, 'tp'), P('tp', None))

    def swap_core(values):
        return lax.ppermute(values, 'tp', [(0, 1), (1, 0), (2, 3), (3, 2)])

    def swap_chip(values):
        return lax.ppermute(values, 'tp', [(0, 2), (2, 0), (1, 3), (3, 1)])

    def with_core(shard, chip, axis):
        return jnp.concatenate([shard, chip, swap_core(shard), swap_core(chip)], axis=axis)

    tie = lax.optimization_barrier

    def local_step(x_tok, y_cap, y_valid, t_emb, mod_table, w_qkv, w_proj, w_cq, w_ckv, w_cproj, w_fc1, w_fc2, d_out):
        width = x_tok.shape[-1]
        me = lax.axis_index('tp')
        batch = x_tok.shape[0] // 4
        rows = x_tok.shape[1]
        local = w_proj.shape[0] * w_proj.shape[1]

        def exchange(values):
            return lax.all_to_all(values, 'tp', split_axis=0, concat_axis=0, tiled=True)

        def own(values):
            return lax.dynamic_slice_in_dim(values, me * batch, batch, axis=0)

        x_own = exchange(x_tok.reshape(4, batch, rows, width))
        qkv_s = w_qkv.transpose(1, 2, 3, 0).reshape(3, local, width)
        qkv_c = swap_chip(qkv_s)
        qkv_w = with_core(qkv_s, qkv_c, 1).reshape(3 * width, width)
        x_own, qkv_w, mid_s = tie((x_own, qkv_w, (
            w_proj.reshape(local, width), w_cq.transpose(1, 2, 0).reshape(local, width),
            w_ckv.transpose(1, 2, 3, 0).reshape(2, local, width), w_cproj.reshape(local, width))))
        mid_c = tuple(swap_chip(shard) for shard in mid_s)

        y_own = own(y_cap)
        n_cap = y_own.shape[1]
        n_pad = -n_cap % 16
        y_own = jnp.pad(y_own, ((0, 0), (0, n_pad), (0, 0)))[None]
        valid = jnp.pad(own(y_valid), ((0, 0), (0, n_pad)))
        key_bias = jnp.where(valid > 0, 0.0, -1e30).astype(F32)
        mod_rows = own(t_emb).astype(F32).reshape(batch, 6, width) + mod_table.astype(F32)
        shift_msa, scale_msa, gate_msa, shift_mlp, scale_mlp, gate_mlp = (mod_rows[:, i, None, :] for i in range(6))

        def dense(values, weight, dim):
            return contract(values.reshape(-1, values.shape[-1]), weight, 1, dim).reshape(
                values.shape[:-1] + (weight.shape[1 - dim],))

        def outer(left, right):
            return contract(left.reshape(-1, left.shape[-1]), right.reshape(-1, right.shape[-1]), 0, 0)

        def over_tokens(values):
            return jnp.sum(values, axis=(0, 2))

        x_res = x_own.astype(F32)
        norm1, inv1 = layer_norm(x_res)
        mod_in1 = (norm1 * (1.0 + scale_msa) + shift_msa).astype(BF16)
        qkv = dense(mod_in1, qkv_w, 1).astype(BF16)
        att_self, lse_self = attn_fwd(qkv, 0, qkv, 1, 2, None)
        mid_w = tuple(with_core(s, c, s.ndim - 2) for s, c in zip(mid_s, mid_c))
        att_self, mid_w, fc1_s, fc2_s = tie((att_self, mid_w, w_fc1, w_fc2))
        proj_w, cq_w, ckv_w, cproj_w = mid_w
        ckv_w = ckv_w.reshape(2 * width, width)
        fc1_c, fc2_c = swap_chip(fc1_s), swap_chip(fc2_s)
        fc1_c, fc2_c, d_tok = tie((fc1_c, fc2_c, d_out))
        d_own = exchange(d_tok.reshape(4, batch, rows, width))
        fc1_w = with_core(fc1_s, fc1_c, 1)
        fc2_w = with_core(fc2_s, fc2_c, 0)
        proj_out = dense(att_self, proj_w, 0).astype(BF16).astype(F32)
        x_one = x_res + gate_msa * proj_out
        cross_in = x_one.astype(BF16)
        q_cross = dense(cross_in, cq_w, 1).astype(BF16)
        kv_cross = dense(y_own, ckv_w, 1).astype(BF16)
        att_cross, lse_cross = attn_fwd(q_cross, 0, kv_cross, 0, 1, key_bias[:, None, :])
        cross_out = dense(att_cross, cproj_w, 0).astype(BF16).astype(F32)
        x_two = x_one + cross_out
        norm2, inv2 = layer_norm(x_two)
        mod_in2 = (norm2 * (1.0 + scale_mlp) + shift_mlp).astype(BF16)
        hidden = dense(mod_in2, fc1_w, 0)
        gelu_out, gelu_pull = jax.vjp(functools.partial(jax.nn.gelu, approximate=True), hidden)
        gelu_out = gelu_out.astype(BF16)

        d_three = d_own.astype(F32)
        d_mlp = (gate_mlp * d_three).astype(BF16)
        d_gelu = dense(d_mlp, fc2_w, 1).astype(BF16)
        d_hidden = gelu_pull(d_gelu.astype(F32))[0].astype(BF16)
        half = gelu_out.shape[-1] // 2
        gelu_out, d_hidden, d_mlp = tie((gelu_out, d_hidden, d_mlp))
        g2 = outer(gelu_out, d_mlp)
        send2 = g2[half:]
        d_hidden, g2, send2 = tie((d_hidden, g2, send2))
        got2 = swap_core(send2)
        g1 = outer(mod_in2, d_hidden)
        send1 = g1[:, half:]
        d_hidden, g1, send1, got2 = tie((d_hidden, g1, send1, got2))
        got1 = swap_core(send1)
        part2 = lax.psum_scatter((g2[:half] + got2).reshape(2, width, width), 'dp', scatter_dimension=1, tiled=True)
        d_mod2 = dense(d_hidden, fc1_w, 1).astype(BF16).astype(F32)
        d_mod2, got1 = tie((d_mod2, got1))
        chip1 = swap_chip(g1[:, width:half] + got1[:, width:])
        d_scale_mlp = over_tokens(d_mod2 * norm2)
        d_shift_mlp = over_tokens(d_mod2)
        d_two = d_three + norm_back(norm2, inv2, d_mod2 * (1.0 + scale_mlp))

        d_cross = d_two.astype(BF16)
        d_att_c = dense(d_cross, cproj_w, 1).astype(BF16)
        dq_cross, d_kv_cross = attn_bwd(q_cross, 0, kv_cross, 0, 1, d_att_c, lse_cross, key_bias[:, :, None], False)
        dq_cross, d_kv_cross, part2, chip1 = tie((dq_cross, d_kv_cross, part2, chip1))
        sum1 = g1[:, :width] + got1[:, :width] + chip1
        d_kv_cross, sum1 = tie((d_kv_cross, sum1))
        g_fc1 = lax.psum(sum1, 'dp')
        chip_part2 = swap_chip(part2[1])
        d_xc = dense(dq_cross, cq_w, 0).astype(BF16).astype(F32)
        d_one = d_two + d_xc
        dy_own = dense(d_kv_cross, ckv_w, 0)[0, :, :n_cap]
        d_proj = (gate_msa * d_one).astype(BF16)
        mid = [head_grad(att_self, d_proj), head_grad(att_cross, d_cross), head_grad(dq_cross, cross_in),
               head_grad(d_kv_cross, y_own)]
        mid_send = jnp.concatenate([grad[1] for grad in mid], axis=1)
        d_proj, mid, mid_send, dy_own = tie((d_proj, mid, mid_send, dy_own))
        mid_got = swap_core(mid_send)
        dy_c = swap_chip(dy_own)
        d_gate_msa = over_tokens(d_one * proj_out)
        d_att_s = dense(d_proj, proj_w, 1).astype(BF16)
        mid_held = jnp.concatenate([grad[0] for grad in mid], axis=1) + mid_got
        sum2 = part2[0] + chip_part2
        d_att_s, mid_held, gelu_late, sum2 = tie((d_att_s, mid_held, gelu_out, sum2))
        mid_part = lax.psum_scatter(mid_held, 'dp', scatter_dimension=1, tiled=True)
        mlp_out = dense(gelu_late, fc2_w, 0).astype(BF16).astype(F32)
        out_own = (x_two + gate_mlp * mlp_out).astype(BF16)
        d_gate_mlp = over_tokens(d_three * mlp_out)
        d_att_s, out_own, sum2, g_fc1 = tie((d_att_s, out_own, sum2, g_fc1))
        g_fc2 = lax.all_gather(sum2, 'dp', axis=0, tiled=True)
        out_tok = exchange(out_own)
        (d_qkv,) = attn_bwd(qkv, 0, qkv, 1, 2, d_att_s, lse_self, None, True)
        grad_qkv = head_grad(d_qkv, mod_in1)
        d_qkv, grad_qkv, dy_c, g_fc2, out_tok = tie((d_qkv, grad_qkv, dy_c, g_fc2, out_tok))
        qkv_got = swap_core(grad_qkv[1])
        d_mod1 = dense(d_qkv, qkv_w, 0).astype(BF16).astype(F32)
        qkv_held = grad_qkv[0] + qkv_got
        d_mod1, qkv_held, mid_part = tie((d_mod1, qkv_held, mid_part))
        qkv_part = lax.psum_scatter(qkv_held, 'dp', scatter_dimension=1, tiled=True)
        mid_chip = swap_chip(mid_part[1])
        d_scale_msa = over_tokens(d_mod1 * norm1)
        d_shift_msa = over_tokens(d_mod1)
        dx_own = (d_one + norm_back(norm1, inv1, d_mod1 * (1.0 + scale_msa))).astype(BF16)
        dx_tok = exchange(dx_own)
        dys = [dy_own, swap_core(dy_own), dy_c, swap_core(dy_c)]
        dy_cap = jnp.zeros((4 * batch,) + dy_own.shape[1:], F32)
        for index, piece in enumerate(dys):
            dy_cap = lax.dynamic_update_slice_in_dim(dy_cap, piece, (me ^ index) * batch, axis=0)
        g_mid = lax.all_gather(mid_part[0] + mid_chip, 'dp', axis=0, tiled=True)
        g_qkv = lax.all_gather(qkv_part[0] + swap_chip(qkv_part[1]), 'dp', axis=0, tiled=True)
        out_tok = out_tok.reshape(x_tok.shape)
        dx_tok = dx_tok.reshape(x_tok.shape)

        d_mods = jnp.stack([d_shift_msa, d_scale_msa, d_gate_msa, d_shift_mlp, d_scale_mlp, d_gate_mlp], axis=1)
        all_mods = lax.all_gather(d_mods, ('dp', 'tp'), axis=0, tiled=True)
        d_table = jnp.sum(all_mods, axis=0)
        dt_emb = lax.dynamic_slice_in_dim(all_mods, lax.axis_index('dp') * 4 * batch, 4 * batch, axis=0)
        dt_emb = dt_emb.reshape(4 * batch, 6 * width)
        n_heads = local // HEAD_DIM

        def heads(grad, lead):
            return grad.reshape(lead, n_heads, HEAD_DIM, width)

        g_proj, g_cproj, g_cq, g_ckv = (g_mid[i * local:(i + count) * local]
                                        for i, count in ((0, 1), (1, 1), (2, 1), (3, 2)))
        return (out_tok, dx_tok, dy_cap, dt_emb, d_table,
                heads(g_qkv, 3).transpose(3, 0, 1, 2), heads(g_proj, 1)[0], heads(g_cq, 1)[0].transpose(2, 0, 1),
                heads(g_ckv, 2).transpose(3, 0, 1, 2), heads(g_cproj, 1)[0], g_fc1, g_fc2)

    return jax.shard_map(local_step, mesh=mesh, in_specs=in_specs, out_specs=out_specs, check_vma=False)
```
